32 devices in a mesh: lat: 2 (over y), lon: 4 (over x, core), lev: 4 (over z).
Axes of the slice: x: 2, y: 2, z: 4, core: 2. Of those that a mesh axis runs over, the one named last changes fastest.
Arguments:
- tracer: float32 [8, 512, 128, 128], P('lat', 'lon', 'lev'), may hold values from 0.5 to 2
- conductance: float32 [8, 512, 128, 128], P('lat', 'lon', 'lev'), may hold values from 0.03 to 0.15
- source: float32 [8, 512, 128, 128], P('lat', 'lon', 'lev'), may hold values from -0.2 to 0.2
Outputs:
- standardized: float32 [8, 512, 128, 128], P('lat', 'lon', 'lev')
- tracer_end: float32 [8, 512, 128, 128], P('lat', 'lon', 'lev')
The draws below stay inside these ranges and needn't reach their ends.
All inputs are finite; a program needn't handle non-finite values.
Results may differ from the reference program's by a relative error of at most 0.00002.
Values sent between devices are 32-bit elements; how exact they have to be, the bound alone decides.
A program may use at most 128 MiB of HBM per device.

```python
import jax
import jax.numpy as jnp
from jax import lax

GRID_J = 8
GRID_I = 512
GRID_K = 128
MEMBERS = 128
STEPS = 3


def shard_levels(stream_key, extent, cuts, smallest, top_value):
    def one(dim, shards_of):
        draws = jax.random.uniform(jax.random.fold_in(jax.random.fold_in(stream_key, 6), dim), (shards_of,), jnp.float32, smallest / len(cuts), top_value / len(cuts))
        return jnp.repeat(jnp.exp(draws), extent[dim] // shards_of).reshape((-1,) + (1,) * (len(extent) - dim - 1))

    level = one(*cuts[0])
    for cut in cuts[1:]:
        level = level * one(*cut)
    return level


def setup_inputs(seed: int = 0) -> dict:
    seeds = jax.random.split(jax.random.key(seed), 4)
    return {
        "tracer": jnp.clip(0.5 + 1.5 * jax.random.uniform(seeds[0], (GRID_J, GRID_I, GRID_K, MEMBERS), jnp.float32) ** shard_levels(seeds[0], (GRID_J, GRID_I, GRID_K, MEMBERS), ((0, 2), (1, 4), (2, 4)), -0.2, 0.2), 0.5, 2.0),
        "conductance": jnp.clip(0.03 + 0.120000007 * jax.random.uniform(seeds[1], (GRID_J, GRID_I, GRID_K, MEMBERS), jnp.float32) ** shard_levels(seeds[1], (GRID_J, GRID_I, GRID_K, MEMBERS), ((0, 2), (1, 4), (2, 4)), -0.2, 0.2), 0.03, 0.15),
        "source": jnp.clip(jax.random.uniform(seeds[2], (GRID_J, GRID_I, GRID_K, MEMBERS), jnp.float32, -0.2, 0.2) * shard_levels(seeds[2], (GRID_J, GRID_I, GRID_K, MEMBERS), ((0, 2), (1, 4), (2, 4)), -0.4, 0.0), -0.2, 0.2),
    }


def inner_cells(values, dims):
    for dim in dims:
        values = lax.slice_in_dim(values, 1, values.shape[dim] - 1, axis=dim)
    return values

def side_cells(values, dim, start, dims):
    others = [other for other in dims if other != dim]
    values = inner_cells(values, others)
    return lax.slice_in_dim(values, start, start + values.shape[dim] - 2, axis=dim)

def advance(padded, conductance, source):
    middle = inner_cells(padded, (0, 1, 2))
    lower = [side_cells(padded, dim, 0, (0, 1, 2)) for dim in (0, 1, 2)]
    upper = [side_cells(padded, dim, 2, (0, 1, 2)) for dim in (0, 1, 2)]
    spread = lower[0] + upper[0] + lower[1] + upper[1] + lower[2] + upper[2] - 6.0 * middle
    return middle + conductance * spread + source

def reference(tracer, conductance, source):
    for step in range(STEPS):
        tracer = advance(jnp.pad(tracer, ((1, 1), (1, 1), (1, 1), (0, 0)), mode='constant'), conductance, source)
    line_mean = lax.optimization_barrier(jnp.mean(tracer, axis=1, keepdims=True))
    centred = tracer - line_mean
    line_variance = lax.optimization_barrier(jnp.mean(centred * centred, axis=1, keepdims=True))
    standardized = centred * lax.rsqrt(line_variance + 0.0001)
    return (standardized, tracer)
```

```python
import functools

import jax
import jax.numpy as jnp
from jax import lax
from jax.experimental import pallas as pl
from jax.experimental.pallas import tpu as pltpu
from jax.sharding import PartitionSpec as P

STEPS = 3
GUESS = 1.0
TILE = 8
ROWS = 8


def kernel(
    sizes, tracer, conductance, source, end, mean_out, scale_out,
    even, odd, cond, sour, z_lower, z_upper, z_first, z_last, sums, peer_sums,
    load_sem, y_send, y_recv, x_send, x_recv, z_send, z_recv, sum_send, sum_recv,
):
    n_lat, n_lon, n_lev = sizes
    J, I, K, M = tracer.shape
    chunks = K // TILE
    blocks = I // ROWS
    count = I * n_lon
    lat, lon, lev = lax.axis_index("lat"), lax.axis_index("lon"), lax.axis_index("lev")
    below = {"lat": lat > 0, "lon": lon > 0, "lev": lev > 0}
    above = {"lat": lat < n_lat - 1, "lon": lon < n_lon - 1, "lev": lev < n_lev - 1}
    index = {"lat": lat, "lon": lon, "lev": lev}
    field = [even, odd]

    def levels(chunk):
        return pl.ds(chunk * TILE, TILE)

    def target(axis, way):
        return {axis: index[axis] + (1 if way == 0 else -1)}

    def y_copy(step, chunk, way):
        plane = J - 1 if way == 0 else 0
        if step == 0:
            src = tracer.at[plane, :, levels(chunk), :]
        else:
            src = field[step % 2].at[plane + 1, pl.ds(1, I), levels(chunk), :]
        dst = field[step % 2].at[0 if way == 0 else J + 1, pl.ds(1, I), levels(chunk), :]
        return pltpu.make_async_remote_copy(
            src_ref=src, dst_ref=dst, send_sem=y_send.at[step, chunk, way],
            recv_sem=y_recv.at[step, chunk, way], device_id=target("lat", way),
            device_id_type=pl.DeviceIdType.MESH)

    def x_copy(step, way):
        buf = field[step % 2]
        return pltpu.make_async_remote_copy(
            src_ref=buf.at[pl.ds(1, J), I if way == 0 else 1],
            dst_ref=buf.at[pl.ds(1, J), 0 if way == 0 else I + 1],
            send_sem=x_send.at[step, way], recv_sem=x_recv.at[step, way],
            device_id=target("lon", way), device_id_type=pl.DeviceIdType.MESH)

    def z_copy(step, way):
        src = z_last if way == 0 else z_first
        dst = z_lower if way == 0 else z_upper
        return pltpu.make_async_remote_copy(
            src_ref=src.at[step % 2], dst_ref=dst.at[step % 2],
            send_sem=z_send.at[step, way], recv_sem=z_recv.at[step, way],
            device_id=target("lev", way), device_id_type=pl.DeviceIdType.MESH)

    def sum_copy(chunk, shift):
        return pltpu.make_async_remote_copy(
            src_ref=sums.at[chunk], dst_ref=peer_sums.at[shift - 1, chunk],
            send_sem=sum_send.at[chunk, shift - 1], recv_sem=sum_recv.at[chunk, shift - 1],
            device_id={"lon": lax.rem(lon + shift, n_lon)}, device_id_type=pl.DeviceIdType.MESH)

    def sends(axis, way, act):
        pl.when((above if way == 0 else below)[axis])(act)

    def arrives(axis, way, act):
        pl.when((below if way == 0 else above)[axis])(act)

    barrier = pltpu.get_barrier_semaphore()
    met = n_lon - 1
    for axis in ("lat", "lev"):
        for way in (0, 1):
            def greet(axis=axis, way=way):
                pl.semaphore_signal(barrier, inc=1, device_id=target(axis, way),
                                    device_id_type=pl.DeviceIdType.MESH)
            sends(axis, way, greet)
        met = met + below[axis].astype(jnp.int32) + above[axis].astype(jnp.int32)
    for shift in range(1, n_lon):
        pl.semaphore_signal(barrier, inc=1, device_id={"lon": lax.rem(lon + shift, n_lon)},
                            device_id_type=pl.DeviceIdType.MESH)

    loads = [
        pltpu.make_async_copy(tracer, even.at[pl.ds(1, J), pl.ds(1, I)], load_sem.at[0]),
        pltpu.make_async_copy(conductance, cond, load_sem.at[1]),
        pltpu.make_async_copy(source, sour, load_sem.at[2]),
    ]
    loads[0].start()
    pl.semaphore_wait(barrier, met)

    for chunk in range(chunks):
        for way in (0, 1):
            sends("lat", way, lambda: y_copy(0, chunk, way).start())
    loads[1].start()
    loads[2].start()

    for way in (0, 1):
        def no_y():
            @pl.loop(0, blocks)
            def _(b):
                for buf in field:
                    buf[0 if way == 0 else J + 1, pl.ds(1 + b * ROWS, ROWS)] = jnp.zeros(
                        (ROWS, K, M), jnp.float32)
        pl.when(jnp.logical_not((below if way == 0 else above)["lat"]))(no_y)

        def no_x():
            for buf in field:
                for j in range(J):
                    buf[1 + j, 0 if way == 0 else I + 1] = jnp.zeros((K, M), jnp.float32)
        pl.when(jnp.logical_not((below if way == 0 else above)["lon"]))(no_x)

        def no_z():
            @pl.loop(0, blocks)
            def _(b):
                for p in range(2):
                    for j in range(J):
                        (z_lower if way == 0 else z_upper)[p, j, pl.ds(b * ROWS, ROWS)] = (
                            jnp.zeros((ROWS, 1, M), jnp.float32))
        pl.when(jnp.logical_not((below if way == 0 else above)["lev"]))(no_z)

    def pack_and_send(step):
        buf = field[step % 2]
        for way in (0, 1):
            sends("lon", way, lambda: x_copy(step, way).start())

        @pl.loop(0, J * blocks)
        def _(q):
            j, r = q // blocks, (q % blocks) * ROWS
            z_first[step % 2, j, pl.ds(r, ROWS)] = buf[1 + j, pl.ds(1 + r, ROWS), pl.ds(0, 1), :]
            z_last[step % 2, j, pl.ds(r, ROWS)] = buf[1 + j, pl.ds(1 + r, ROWS), pl.ds(K - 1, 1), :]

        for way in (0, 1):
            sends("lev", way, lambda: z_copy(step, way).start())

    def next_rows(step, chunk, j, r):
        buf = field[step % 2]
        here = levels(chunk)
        mid = buf[1 + j, pl.ds(1 + r, ROWS), here, :]
        k = lax.broadcasted_iota(jnp.int32, mid.shape, 1)
        if chunk == 0:
            edge = jnp.broadcast_to(z_lower[step % 2, j, pl.ds(r, ROWS)], mid.shape)
        else:
            edge = pltpu.roll(buf[1 + j, pl.ds(1 + r, ROWS), levels(chunk - 1), :], 1, 1)
        k_lower = jnp.where(k == 0, edge, pltpu.roll(mid, 1, 1))
        if chunk == chunks - 1:
            edge = jnp.broadcast_to(z_upper[step % 2, j, pl.ds(r, ROWS)], mid.shape)
        else:
            edge = pltpu.roll(buf[1 + j, pl.ds(1 + r, ROWS), levels(chunk + 1), :], TILE - 1, 1)
        k_upper = jnp.where(k == TILE - 1, edge, pltpu.roll(mid, TILE - 1, 1))
        spread = (
            buf[j, pl.ds(1 + r, ROWS), here, :] + buf[2 + j, pl.ds(1 + r, ROWS), here, :]
            + buf[1 + j, pl.ds(r, ROWS), here, :] + buf[1 + j, pl.ds(2 + r, ROWS), here, :]
            + k_lower + k_upper - 6.0 * mid)
        return mid + cond[j, pl.ds(r, ROWS), here, :] * spread + sour[j, pl.ds(r, ROWS), here, :]

    def planes(step, chunk, first, number):
        if step < STEPS - 1:
            to = field[(step + 1) % 2]

            @pl.loop(0, number * blocks)
            def _(q):
                j, r = first + q // blocks, (q % blocks) * ROWS
                to[1 + j, pl.ds(1 + r, ROWS), levels(chunk), :] = next_rows(step, chunk, j, r)
        else:
            @pl.loop(0, number)
            def _(p):
                j = first + p

                def body(b, totals):
                    new = next_rows(step, chunk, j, b * ROWS)
                    end[j, pl.ds(b * ROWS, ROWS), levels(chunk), :] = new
                    moved = new - GUESS
                    return (totals[0] + jnp.sum(moved, axis=0),
                            totals[1] + jnp.sum(moved * moved, axis=0))

                zero = jnp.zeros((TILE, M), jnp.float32)
                total, square = lax.fori_loop(0, blocks, body, (zero, zero))
                sums[chunk, 0, j] = total
                sums[chunk, 1, j] = square

    def y_arrives(step, chunk, way):
        arrives("lat", way, lambda: y_copy(step, chunk, way).wait_recv())

    early = jnp.where(lat == 0, 0, J - 1)
    late = J - 1 - early

    loads[0].wait()
    pack_and_send(0)
    loads[1].wait()
    loads[2].wait()
    for step in range(STEPS):
        if step >= 1:
            for way in (0, 1):
                sends("lon", way, lambda: x_copy(step - 1, way).wait_send())
                sends("lev", way, lambda: z_copy(step - 1, way).wait_send())
                for chunk in range(chunks):
                    sends("lat", way, lambda: y_copy(step - 1, chunk, way).wait_send())
        for way in (0, 1):
            arrives("lon", way, lambda: x_copy(step, way).wait_recv())
            arrives("lev", way, lambda: z_copy(step, way).wait_recv())
        if step == STEPS - 1:
            for chunk in range(chunks):
                planes(step, chunk, 1, J - 2)
        for chunk in range(chunks):
            if step < STEPS - 1:
                planes(step, chunk, 1, J - 2)
            pl.when(jnp.logical_and(lat > 0, lat < n_lat - 1))(
                lambda: y_copy(step, chunk, 1).wait_recv())
            planes(step, chunk, early, 1)
            pl.when(lat > 0)(lambda: y_copy(step, chunk, 0).wait_recv())
            pl.when(jnp.logical_and(lat == 0, lat < n_lat - 1))(
                lambda: y_copy(step, chunk, 1).wait_recv())
            planes(step, chunk, late, 1)
            if step < STEPS - 1:
                for way in (0, 1):
                    sends("lat", way, lambda: y_copy(step + 1, chunk, way).start())
            else:
                for shift in range(1, n_lon):
                    sum_copy(chunk, shift).start()
        if step < STEPS - 1:
            pack_and_send(step + 1)

    for chunk in range(chunks):
        for shift in range(1, n_lon):
            sum_copy(chunk, shift).wait_recv()
        total = sums[chunk]
        for shift in range(1, n_lon):
            total = total + peer_sums[shift - 1, chunk]
        offset = total[0] / count
        variance = total[1] / count - offset * offset
        mean_out[:, levels(chunk), :] = GUESS + offset
        scale_out[:, levels(chunk), :] = lax.rsqrt(variance + 0.0001)

    for chunk in range(chunks):
        for shift in range(1, n_lon):
            sum_copy(chunk, shift).wait_send()
        for way in (0, 1):
            sends("lat", way, lambda: y_copy(STEPS - 1, chunk, way).wait_send())
    for way in (0, 1):
        sends("lon", way, lambda: x_copy(STEPS - 1, way).wait_send())
        sends("lev", way, lambda: z_copy(STEPS - 1, way).wait_send())


def shards(sizes, tracer, conductance, source):
    n_lat, n_lon, n_lev = sizes
    J, I, K, M = tracer.shape
    chunks = K // TILE
    f32 = jnp.float32
    dma = pltpu.SemaphoreType.DMA
    peers = max(n_lon - 1, 1)
    end, mean, scale = pl.pallas_call(
        functools.partial(kernel, sizes),
        out_shape=[
            pltpu.VMEM((J, I, K, M), f32),
            jax.ShapeDtypeStruct((J, K, M), f32),
            jax.ShapeDtypeStruct((J, K, M), f32),
        ],
        in_specs=[pl.BlockSpec(memory_space=pltpu.HBM)] * 3,
        out_specs=[pl.BlockSpec(memory_space=pltpu.VMEM)] * 3,
        scratch_shapes=[
            pltpu.VMEM((J + 2, I + 2, K, M), f32),
            pltpu.VMEM((J + 2, I + 2, K, M), f32),
            pltpu.VMEM((J, I, K, M), f32),
            pltpu.VMEM((J, I, K, M), f32),
            pltpu.VMEM((2, J, I, 1, M), f32),
            pltpu.VMEM((2, J, I, 1, M), f32),
            pltpu.VMEM((2, J, I, 1, M), f32),
            pltpu.VMEM((2, J, I, 1, M), f32),
            pltpu.VMEM((chunks, 2, J, TILE, M), f32),
            pltpu.VMEM((peers, chunks, 2, J, TILE, M), f32),
            dma((3,)),
            dma((STEPS, chunks, 2)),
            dma((STEPS, chunks, 2)),
            dma((STEPS, 2)),
            dma((STEPS, 2)),
            dma((STEPS, 2)),
            dma((STEPS, 2)),
            dma((chunks, peers)),
            dma((chunks, peers)),
        ],
        compiler_params=pltpu.CompilerParams(
            collective_id=0, has_side_effects=True, vmem_limit_bytes=47 * 1024 * 1024),
    )(tracer, conductance, source)
    standardized = (end - mean[:, None]) * scale[:, None]
    return (standardized, end)


def solution(mesh):
    placed = P("lat", "lon", "lev", None)
    sizes = tuple(mesh.shape[axis] for axis in ("lat", "lon", "lev"))
    return jax.shard_map(
        functools.partial(shards, sizes),
        mesh=mesh,
        in_specs=(placed, placed, placed),
        out_specs=(placed, placed),
        check_vma=False,
    )
```

```python
import functools

import jax
import jax.numpy as jnp
from jax import lax
from jax.experimental import pallas as pl
from jax.experimental.pallas import tpu as pltpu
from jax.sharding import PartitionSpec as P

STEPS = 3
GUESS = 1.0
TILE = 8
ROWS = 8


def kernel(
    sizes, tracer, conductance, source, end, mean_out, scale_out,
    even, odd, cond, sour, z_lower, z_upper, z_first, z_last, sums, peer_sums,
    load_sem, y_send, y_recv, x_send, x_recv, z_send, z_recv, sum_send, sum_recv,
):
    n_lat, n_lon, n_lev = sizes
    J, I, K, M = tracer.shape
    chunks = K // TILE
    blocks = I // ROWS
    count = I * n_lon
    lat, lon, lev = lax.axis_index("lat"), lax.axis_index("lon"), lax.axis_index("lev")
    below = {"lat": lat > 0, "lon": lon > 0, "lev": lev > 0}
    above = {"lat": lat < n_lat - 1, "lon": lon < n_lon - 1, "lev": lev < n_lev - 1}
    index = {"lat": lat, "lon": lon, "lev": lev}
    field = [even, odd]

    def levels(chunk):
        return pl.ds(chunk * TILE, TILE)

    def target(axis, way):
        return {axis: index[axis] + (1 if way == 0 else -1)}

    def y_copy(step, chunk, way):
        plane = J - 1 if way == 0 else 0
        if step == 0:
            src = tracer.at[plane, :, levels(chunk), :]
        else:
            src = field[step % 2].at[plane + 1, pl.ds(1, I), levels(chunk), :]
        dst = field[step % 2].at[0 if way == 0 else J + 1, pl.ds(1, I), levels(chunk), :]
        return pltpu.make_async_remote_copy(
            src_ref=src, dst_ref=dst, send_sem=y_send.at[step, chunk, way],
            recv_sem=y_recv.at[step, chunk, way], device_id=target("lat", way),
            device_id_type=pl.DeviceIdType.MESH)

    def x_copy(step, way):
        buf = field[step % 2]
        return pltpu.make_async_remote_copy(
            src_ref=buf.at[pl.ds(1, J), I if way == 0 else 1],
            dst_ref=buf.at[pl.ds(1, J), 0 if way == 0 else I + 1],
            send_sem=x_send.at[step, way], recv_sem=x_recv.at[step, way],
            device_id=target("lon", way), device_id_type=pl.DeviceIdType.MESH)

    def z_copy(step, way):
        src = z_last if way == 0 else z_first
        dst = z_lower if way == 0 else z_upper
        return pltpu.make_async_remote_copy(
            src_ref=src.at[step % 2], dst_ref=dst.at[step % 2],
            send_sem=z_send.at[step, way], recv_sem=z_recv.at[step, way],
            device_id=target("lev", way), device_id_type=pl.DeviceIdType.MESH)

    early = jnp.where(lat == 0, 0, J - 1)
    late = J - 1 - early
    parts = [pl.ds(jnp.where(lat == 0, 0, 1), J - 1), pl.ds(late, 1)]

    def sum_copy(chunk, shift, part):
        return pltpu.make_async_remote_copy(
            src_ref=sums.at[chunk, parts[part]],
            dst_ref=peer_sums.at[shift - 1, chunk, parts[part]],
            send_sem=sum_send.at[chunk, shift - 1, part],
            recv_sem=sum_recv.at[chunk, shift - 1, part],
            device_id={"lon": lax.rem(lon + shift, n_lon)}, device_id_type=pl.DeviceIdType.MESH)

    def sends(axis, way, act):
        pl.when((above if way == 0 else below)[axis])(act)

    def arrives(axis, way, act):
        pl.when((below if way == 0 else above)[axis])(act)

    barrier = pltpu.get_barrier_semaphore()
    met = n_lon - 1
    for axis in ("lat", "lev"):
        for way in (0, 1):
            def greet(axis=axis, way=way):
                pl.semaphore_signal(barrier, inc=1, device_id=target(axis, way),
                                    device_id_type=pl.DeviceIdType.MESH)
            sends(axis, way, greet)
        met = met + below[axis].astype(jnp.int32) + above[axis].astype(jnp.int32)
    for shift in range(1, n_lon):
        pl.semaphore_signal(barrier, inc=1, device_id={"lon": lax.rem(lon + shift, n_lon)},
                            device_id_type=pl.DeviceIdType.MESH)

    loads = [
        pltpu.make_async_copy(tracer, even.at[pl.ds(1, J), pl.ds(1, I)], load_sem.at[0]),
        pltpu.make_async_copy(conductance, cond, load_sem.at[1]),
        pltpu.make_async_copy(source, sour, load_sem.at[2]),
    ]
    loads[0].start()
    pl.semaphore_wait(barrier, met)

    for chunk in range(chunks):
        for way in (0, 1):
            sends("lat", way, lambda: y_copy(0, chunk, way).start())
    loads[1].start()
    loads[2].start()

    for way in (0, 1):
        def no_y():
            @pl.loop(0, blocks)
            def _(b):
                for buf in field:
                    buf[0 if way == 0 else J + 1, pl.ds(1 + b * ROWS, ROWS)] = jnp.zeros(
                        (ROWS, K, M), jnp.float32)
        pl.when(jnp.logical_not((below if way == 0 else above)["lat"]))(no_y)

        def no_x():
            for buf in field:
                for j in range(J):
                    buf[1 + j, 0 if way == 0 else I + 1] = jnp.zeros((K, M), jnp.float32)
        pl.when(jnp.logical_not((below if way == 0 else above)["lon"]))(no_x)

        def no_z():
            @pl.loop(0, blocks)
            def _(b):
                for p in range(2):
                    for j in range(J):
                        (z_lower if way == 0 else z_upper)[p, j, pl.ds(b * ROWS, ROWS)] = (
                            jnp.zeros((ROWS, 1, M), jnp.float32))
        pl.when(jnp.logical_not((below if way == 0 else above)["lev"]))(no_z)

    def pack_and_send(step):
        buf = field[step % 2]
        for way in (0, 1):
            sends("lon", way, lambda: x_copy(step, way).start())

        @pl.loop(0, J * blocks)
        def _(q):
            j, r = q // blocks, (q % blocks) * ROWS
            z_first[step % 2, j, pl.ds(r, ROWS)] = buf[1 + j, pl.ds(1 + r, ROWS), pl.ds(0, 1), :]
            z_last[step % 2, j, pl.ds(r, ROWS)] = buf[1 + j, pl.ds(1 + r, ROWS), pl.ds(K - 1, 1), :]

        for way in (0, 1):
            sends("lev", way, lambda: z_copy(step, way).start())

    def next_rows(step, chunk, j, r):
        buf = field[step % 2]
        here = levels(chunk)
        mid = buf[1 + j, pl.ds(1 + r, ROWS), here, :]
        k = lax.broadcasted_iota(jnp.int32, mid.shape, 1)
        if chunk == 0:
            edge = jnp.broadcast_to(z_lower[step % 2, j, pl.ds(r, ROWS)], mid.shape)
        else:
            edge = pltpu.roll(buf[1 + j, pl.ds(1 + r, ROWS), levels(chunk - 1), :], 1, 1)
        k_lower = jnp.where(k == 0, edge, pltpu.roll(mid, 1, 1))
        if chunk == chunks - 1:
            edge = jnp.broadcast_to(z_upper[step % 2, j, pl.ds(r, ROWS)], mid.shape)
        else:
            edge = pltpu.roll(buf[1 + j, pl.ds(1 + r, ROWS), levels(chunk + 1), :], TILE - 1, 1)
        k_upper = jnp.where(k == TILE - 1, edge, pltpu.roll(mid, TILE - 1, 1))
        spread = (
            buf[j, pl.ds(1 + r, ROWS), here, :] + buf[2 + j, pl.ds(1 + r, ROWS), here, :]
            + buf[1 + j, pl.ds(r, ROWS), here, :] + buf[1 + j, pl.ds(2 + r, ROWS), here, :]
            + k_lower + k_upper - 6.0 * mid)
        return mid + cond[j, pl.ds(r, ROWS), here, :] * spread + sour[j, pl.ds(r, ROWS), here, :]

    def planes(step, chunk, first, number):
        if step < STEPS - 1:
            to = field[(step + 1) % 2]

            @pl.loop(0, number * blocks)
            def _(q):
                j, r = first + q // blocks, (q % blocks) * ROWS
                to[1 + j, pl.ds(1 + r, ROWS), levels(chunk), :] = next_rows(step, chunk, j, r)
        else:
            @pl.loop(0, number)
            def _(p):
                j = first + p

                def body(b, totals):
                    new = next_rows(step, chunk, j, b * ROWS)
                    end[j, pl.ds(b * ROWS, ROWS), levels(chunk), :] = new
                    moved = new - GUESS
                    return (totals[0] + jnp.sum(moved, axis=0),
                            totals[1] + jnp.sum(moved * moved, axis=0))

                zero = jnp.zeros((TILE, M), jnp.float32)
                total, square = lax.fori_loop(0, blocks, body, (zero, zero))
                sums[chunk, j, 0] = total
                sums[chunk, j, 1] = square

    def y_arrives(step, chunk, way):
        arrives("lat", way, lambda: y_copy(step, chunk, way).wait_recv())

    loads[0].wait()
    pack_and_send(0)
    loads[1].wait()
    loads[2].wait()
    for step in range(STEPS):
        if step >= 1:
            for way in (0, 1):
                sends("lon", way, lambda: x_copy(step - 1, way).wait_send())
                sends("lev", way, lambda: z_copy(step - 1, way).wait_send())
                for chunk in range(chunks):
                    sends("lat", way, lambda: y_copy(step - 1, chunk, way).wait_send())
        for way in (0, 1):
            arrives("lon", way, lambda: x_copy(step, way).wait_recv())
            arrives("lev", way, lambda: z_copy(step, way).wait_recv())
        if step == STEPS - 1:
            for chunk in range(chunks):
                planes(step, chunk, 1, J - 2)
        for chunk in range(chunks):
            if step < STEPS - 1:
                planes(step, chunk, 1, J - 2)
            pl.when(jnp.logical_and(lat > 0, lat < n_lat - 1))(
                lambda: y_copy(step, chunk, 1).wait_recv())
            planes(step, chunk, early, 1)
            if step == STEPS - 1:
                for shift in range(1, n_lon):
                    sum_copy(chunk, shift, 0).start()
            pl.when(lat > 0)(lambda: y_copy(step, chunk, 0).wait_recv())
            pl.when(jnp.logical_and(lat == 0, lat < n_lat - 1))(
                lambda: y_copy(step, chunk, 1).wait_recv())
            planes(step, chunk, late, 1)
            if step < STEPS - 1:
                for way in (0, 1):
                    sends("lat", way, lambda: y_copy(step + 1, chunk, way).start())
            else:
                for shift in range(1, n_lon):
                    sum_copy(chunk, shift, 1).start()
        if step < STEPS - 1:
            pack_and_send(step + 1)

    for chunk in range(chunks):
        for shift in range(1, n_lon):
            for part in (0, 1):
                sum_copy(chunk, shift, part).wait_recv()
        total = sums[chunk]
        for shift in range(1, n_lon):
            total = total + peer_sums[shift - 1, chunk]
        offset = total[:, 0] / count
        variance = total[:, 1] / count - offset * offset
        mean_out[:, levels(chunk), :] = GUESS + offset
        scale_out[:, levels(chunk), :] = lax.rsqrt(variance + 0.0001)

    for chunk in range(chunks):
        for shift in range(1, n_lon):
            for part in (0, 1):
                sum_copy(chunk, shift, part).wait_send()
        for way in (0, 1):
            sends("lat", way, lambda: y_copy(STEPS - 1, chunk, way).wait_send())
    for way in (0, 1):
        sends("lon", way, lambda: x_copy(STEPS - 1, way).wait_send())
        sends("lev", way, lambda: z_copy(STEPS - 1, way).wait_send())


def write_out(end, mean, scale, standardized, end_out, held, sem):
    J, I, K, M = end.shape
    keep = pltpu.make_async_copy(end, end_out, sem.at[J])
    keep.start()
    copies = []
    for j in range(J):
        offset, factor = mean[j], scale[j]

        @pl.loop(0, I // ROWS)
        def _(b):
            rows = pl.ds(b * ROWS, ROWS)
            held[j, rows] = (end[j, rows] - offset) * factor

        copies.append(pltpu.make_async_copy(held.at[j], standardized.at[j], sem.at[j]))
        copies[-1].start()
    for copy in copies + [keep]:
        copy.wait()


def shards(sizes, tracer, conductance, source):
    n_lat, n_lon, n_lev = sizes
    J, I, K, M = tracer.shape
    chunks = K // TILE
    f32 = jnp.float32
    dma = pltpu.SemaphoreType.DMA
    peers = max(n_lon - 1, 1)
    end, mean, scale = pl.pallas_call(
        functools.partial(kernel, sizes),
        out_shape=[
            pltpu.VMEM((J, I, K, M), f32),
            pltpu.VMEM((J, K, M), f32),
            pltpu.VMEM((J, K, M), f32),
        ],
        in_specs=[pl.BlockSpec(memory_space=pltpu.HBM)] * 3,
        out_specs=[pl.BlockSpec(memory_space=pltpu.VMEM)] * 3,
        scratch_shapes=[
            pltpu.VMEM((J + 2, I + 2, K, M), f32),
            pltpu.VMEM((J + 2, I + 2, K, M), f32),
            pltpu.VMEM((J, I, K, M), f32),
            pltpu.VMEM((J, I, K, M), f32),
            pltpu.VMEM((2, J, I, 1, M), f32),
            pltpu.VMEM((2, J, I, 1, M), f32),
            pltpu.VMEM((2, J, I, 1, M), f32),
            pltpu.VMEM((2, J, I, 1, M), f32),
            pltpu.VMEM((chunks, J, 2, TILE, M), f32),
            pltpu.VMEM((peers, chunks, J, 2, TILE, M), f32),
            dma((3,)),
            dma((STEPS, chunks, 2)),
            dma((STEPS, chunks, 2)),
            dma((STEPS, 2)),
            dma((STEPS, 2)),
            dma((STEPS, 2)),
            dma((STEPS, 2)),
            dma((chunks, peers, 2)),
            dma((chunks, peers, 2)),
        ],
        compiler_params=pltpu.CompilerParams(
            collective_id=0, has_side_effects=True, vmem_limit_bytes=47 * 1024 * 1024),
    )(tracer, conductance, source)
    return pl.pallas_call(
        write_out,
        out_shape=[jax.ShapeDtypeStruct((J, I, K, M), f32)] * 2,
        in_specs=[pl.BlockSpec(memory_space=pltpu.VMEM)] * 3,
        out_specs=[pl.BlockSpec(memory_space=pltpu.HBM)] * 2,
        scratch_shapes=[pltpu.VMEM((J, I, K, M), f32), dma((J + 1,))],
        compiler_params=pltpu.CompilerParams(vmem_limit_bytes=32 * 1024 * 1024),
    )(end, mean, scale)


def solution(mesh):
    placed = P("lat", "lon", "lev", None)
    sizes = tuple(mesh.shape[axis] for axis in ("lat", "lon", "lev"))
    return jax.shard_map(
        functools.partial(shards, sizes),
        mesh=mesh,
        in_specs=(placed, placed, placed),
        out_specs=(placed, placed),
        check_vma=False,
    )
```
